512 devices in a mesh: dp: 256 (over z, x, y), mp: 2 (over core).
Axes of the slice: x: 4, y: 8, z: 8, core: 2. Of those that a mesh axis runs over, the one named last changes fastest.
Arguments:
- normed: bfloat16 [98304, 2048], P(('dp', 'mp')), may hold values from -24 to 24
- key_grad: bfloat16 [98304, 512], P('dp', 'mp'), may hold values from -0.01953125 to 0.01953125
- stale: bfloat16 [256, 2048, 512], P('dp', None, 'mp'), may hold values from -0.375 to 0.375
- worker_flag: int32 [256], P('dp'), may hold values 0 or 1
- block_mask: int32 [256, 4], P('dp'), may hold values 0 or 1
- aggregate: float32 [2048, 512], P('dp', 'mp'), may hold values from -6 to 6
- master: float32 [2048, 512], P('dp', 'mp'), may hold values from -0.125 to 0.125
- moment_one: float32 [2048, 512], P('dp', 'mp'), may hold values from -6 to 6
- moment_two: float32 [2048, 512], P('dp', 'mp'), may hold values from 0.5 to 4
Outputs:
- new_aggregate: float32 [2048, 512], P('dp', 'mp')
- new_master: float32 [2048, 512], P('dp', 'mp')
- new_moment_one: float32 [2048, 512], P('dp', 'mp')
- new_moment_two: float32 [2048, 512], P('dp', 'mp')
- weights: bfloat16 [2048, 512], P(None, 'mp')
- new_stale: bfloat16 [256, 2048, 512], P('dp', None, 'mp')
The draws below stay inside these ranges and needn't reach their ends.
All inputs are finite; a program needn't handle non-finite values. No bound on the sum of `worker_flag` on one device may be relied on, other than what follows from the above.
Results may differ from the reference program's by a relative error of at most 0.0004.
Values may be sent and summed in bfloat16 or wider, within the bound.
No kernel may reach another device: no remote copies, remote signals or barrier semaphores. Data moves between devices by JAX's collectives and lax.ppermute only.
A program may use at most 64 MiB of HBM per device.

```python
import math
import jax
import jax.numpy as jnp
from jax import lax

D = 2048
H = 512
BLOCKS = 4
STEP = 10
TOK_DEV = 384
TOKENS = 98304
N_DP = 256


def place_ends(values, key, least, largest):
    extent = values.shape
    index_at = [jax.random.randint(jax.random.fold_in(key, axis), (), 0, extent[axis]) for axis in range(len(extent))]
    values = values.at[tuple(index_at)].set(least)
    longest = extent.index(max(extent))
    index_at[longest] = (index_at[longest] + 1) % extent[longest]
    return values.at[tuple(index_at)].set(largest)


def with_spikes(array, own_key, source, target, blocks, factor):
    def block_of(dim):
        return (jnp.arange(array.shape[dim]) // (array.shape[dim] // blocks)).reshape((-1,) + (1,) * (array.ndim - 1 - dim))

    near = jax.random.permutation(own_key, blocks)[block_of(target)]
    far = (block_of(target) + blocks // 2) % blocks
    return jnp.where((block_of(source) == near) | (block_of(source) == far), factor * array, array)


def block_scale(rng, dims, split, smallest, high):
    level, own = 1.0, jax.random.fold_in(rng, 6)
    for dim, parts in split:
        draws = jnp.exp(jax.random.uniform(jax.random.fold_in(own, dim), (parts,), jnp.float32, smallest / len(split), high / len(split)))
        level = level * jnp.repeat(draws, dims[dim] // parts).reshape([-1 if axis == dim else 1 for axis in range(len(dims))])
    return level


def normal_values(stream_key, extent, width, bound, shards=(), held_as=jnp.bfloat16):
    loudness = block_scale(stream_key, extent, shards, -0.22, 0.18) if shards else 1.0
    drawn = jax.random.normal(stream_key, extent, jnp.float32) * width * loudness
    return jnp.minimum(jnp.maximum(drawn, -bound), bound).astype(held_as)


def bell_draw_with(rng, shape, spread, most, cuts, heavy, kind=jnp.bfloat16):
    entries = spread * jax.random.normal(rng, shape, jnp.float32)
    if cuts:
        entries = entries * block_scale(rng, shape, cuts, -0.22, 0.18)
    return jnp.clip(with_spikes(entries, jax.random.fold_in(rng, 3), *heavy), -most, most).astype(kind)


def setup_inputs(seed: int = 0) -> dict:
    streams_of = jax.random.split(jax.random.key(seed), 10)
    return {
        "normed": bell_draw_with(streams_of[0], (TOKENS, D), 1.0, 24.0, ((0, 512),), (0, 1, 512, 6.0)),
        "key_grad": normal_values(streams_of[1], (TOKENS, H), ((TOK_DEV * N_DP) ** -0.5), 0.01953125, ((0, 256), (1, 2))),
        "stale": normal_values(streams_of[2], (N_DP, D, H), (N_DP ** -0.5), 0.375, ((0, 256), (2, 2))),
        "worker_flag": place_ends((jax.random.randint(streams_of[3], (N_DP,), 0, 2) < 1).astype(jnp.int32), jax.random.fold_in(streams_of[3], 1), 0, 1),
        "block_mask": place_ends((jax.random.randint(streams_of[4], (N_DP, BLOCKS), 0, 3) < 2).astype(jnp.int32), jax.random.fold_in(streams_of[4], 1), 0, 1),
        "aggregate": normal_values(streams_of[5], (D, H), 1.0, 6.0, ((0, 256), (1, 2)), jnp.float32),
        "master": normal_values(streams_of[6], (D, H), 0.02, 0.125, ((0, 256), (1, 2)), jnp.float32),
        "moment_one": normal_values(streams_of[7], (D, H), 1.0, 6.0, ((0, 256), (1, 2)), jnp.float32),
        "moment_two": jnp.clip(jnp.exp(math.log(4.0) - 2.0794415 * jax.random.uniform(streams_of[8], (D, H), jnp.float32) ** block_scale(streams_of[8], (D, H), ((0, 256), (1, 2)), -0.2, 0.2)), 0.5, 4.0),
    }


beta_one = 0.9
beta_two = 0.95
learn_rate = 0.001
decay_rate = 0.1
epsilon = 1e-08

def reference(normed, key_grad, stale, worker_flag, block_mask, aggregate, master, moment_one, moment_two):
    column_block = jnp.arange(H, dtype=jnp.int32) // (H // BLOCKS)
    onehot = (column_block[:, None] == jnp.arange(BLOCKS, dtype=jnp.int32)[None, :]).astype(jnp.int32)
    per_column = lax.optimization_barrier(jnp.sum(block_mask[:, None, :] * onehot[None, :, :], axis=2))
    trig_all = worker_flag[:, None] * per_column
    in_rows = normed.reshape(N_DP, TOK_DEV, D)
    out_rows = key_grad.reshape(N_DP, TOK_DEV, H)

    def one_worker(total, items):
        inputs, grad_out, old, trig = items
        grad = lax.dot_general(inputs, grad_out, (((0,), (0,)), ((), ())), preferred_element_type=jnp.float32)
        weight = trig.astype(jnp.float32)
        total = total + weight[None, :] * (grad - old.astype(jnp.float32))
        kept = jnp.where(trig[None, :] > 0, grad.astype(jnp.bfloat16), old)
        return (total, kept)
    summed, new_stale = lax.scan(one_worker, jnp.zeros((D, H), jnp.float32), (in_rows, out_rows, stale, trig_all))
    new_aggregate = aggregate + summed
    grads = new_aggregate
    new_moment_one = beta_one * moment_one + (1.0 - beta_one) * grads
    new_moment_two = beta_two * moment_two + (1.0 - beta_two) * grads * grads
    first_hat = new_moment_one / (1.0 - beta_one ** STEP)
    second_hat = new_moment_two / (1.0 - beta_two ** STEP)
    update = first_hat / (jnp.sqrt(second_hat) + epsilon)
    new_master = master - learn_rate * (update + decay_rate * master)
    weights = new_master.astype(jnp.bfloat16)
    return (new_aggregate, new_master, new_moment_one, new_moment_two, weights, new_stale)
```

```python
import jax
import jax.numpy as jnp
from jax import lax
from jax.experimental.layout import Layout, with_layout_constraint
from jax.sharding import Mesh
from jax.sharding import PartitionSpec as P

H = 512
BLOCKS = 4
STEP = 10
DP = ("zh", "zl", "x", "yh", "yl")
NEAR = ('x', 'yl')
FAR = ('zh', 'zl', 'yh')
NEAR_BACK = ('x', 'yl')
FAR_BACK = ('zh', 'zl', 'yh')
SCALE_ONE = 256.0
SCALE_TWO = 32.0

beta_one = 0.9
beta_two = 0.95
learn_rate = 0.001
decay_rate = 0.1
epsilon = 1e-08


def product(rows, cols):
    return lax.dot_general(rows, cols, (((0,), (0,)), ((), ())), preferred_element_type=jnp.float32)


def on_device(
    normed, key_grad, stale, worker_flag, block_mask, aggregate, master, moment_one, moment_two
):
    rows, half_cols = normed.shape[0], key_grad.shape[1]
    core = lax.axis_index("mp")
    first_col = core * half_cols
    columns = first_col + jnp.arange(half_cols, dtype=jnp.int32)
    column_block = columns // (H // BLOCKS)
    onehot = (column_block[:, None] == jnp.arange(BLOCKS, dtype=jnp.int32)[None, :]).astype(
        jnp.int32
    )
    trig = worker_flag[0] * jnp.sum(onehot * block_mask[0][None, :], axis=1)
    weight = trig.astype(jnp.float32) * SCALE_ONE
    other = lax.ppermute(normed, "mp", [(0, 1), (1, 0)])
    own_part = product(normed, lax.dynamic_slice_in_dim(key_grad, core * rows, rows, 0))
    grad = own_part + product(
        other, lax.dynamic_slice_in_dim(key_grad, (1 - core) * rows, rows, 0)
    )
    grad = with_layout_constraint(grad, Layout((0, 1)))
    old = stale[0]
    term = (weight[None, :] * (grad - old.astype(jnp.float32))).astype(jnp.float16)
    d = term.shape[0]
    sizes = tuple(lax.axis_size(a) for a in DP)
    n_near, n_far = lax.axis_size(NEAR), lax.axis_size(FAR)
    own = d // (n_near * n_far)
    order = [DP.index(a) for a in NEAR + FAR]
    pieces = term.reshape(*sizes, own, half_cols).transpose(*order, len(DP), len(DP) + 1)
    pieces = pieces.reshape(n_near, n_far * own, half_cols)
    near = lax.all_to_all(pieces, NEAR, 0, 0, tiled=True)
    partial = jnp.sum(near.astype(jnp.float32), axis=0) * (SCALE_TWO / SCALE_ONE)
    partial = partial.astype(jnp.float16).reshape(n_far, own, half_cols)
    far = lax.all_to_all(partial, FAR, 0, 0, tiled=True)
    reduced = jnp.sum(far.astype(jnp.float32), axis=0) * (1.0 / SCALE_TWO)
    new_aggregate = aggregate + reduced
    new_moment_one = beta_one * moment_one + (1.0 - beta_one) * new_aggregate
    new_moment_two = beta_two * moment_two + (1.0 - beta_two) * new_aggregate * new_aggregate
    first_hat = new_moment_one / (1.0 - beta_one**STEP)
    second_hat = new_moment_two / (1.0 - beta_two**STEP)
    update = first_hat / (jnp.sqrt(second_hat) + epsilon)
    new_master = master - learn_rate * (update + decay_rate * master)
    fresh = new_master.astype(jnp.bfloat16)
    n_near, n_far = lax.axis_size(NEAR_BACK), lax.axis_size(FAR_BACK)
    copies = jnp.broadcast_to(fresh, (n_far, own, half_cols))
    block = lax.all_to_all(copies, FAR_BACK, 0, 0, tiled=True).reshape(n_far * own, half_cols)
    copies = jnp.broadcast_to(block, (n_near, *block.shape))
    weights = lax.all_to_all(copies, NEAR_BACK, 0, 0, tiled=True)
    back = NEAR_BACK + FAR_BACK
    weights = weights.reshape(*(lax.axis_size(a) for a in back), own, half_cols)
    weights = weights.transpose(*(back.index(a) for a in DP), len(DP), len(DP) + 1)
    weights = weights.reshape(d, half_cols)
    kept = jnp.where(trig[None, :] > 0, grad.astype(jnp.bfloat16), old)
    return (new_aggregate, new_master, new_moment_one, new_moment_two, weights, kept[None])


def solution(mesh):
    torus = Mesh(mesh.devices.reshape(4, 2, 4, 4, 2, mesh.shape["mp"]), (*DP, "mp"))
    return jax.shard_map(
        on_device,
        mesh=torus,
        in_specs=(
            P((*DP, "mp"), None),
            P(DP, "mp"),
            P(DP, None, "mp"),
            P(DP),
            P(DP, None),
            P(DP, "mp"),
            P(DP, "mp"),
            P(DP, "mp"),
            P(DP, "mp"),
        ),
        out_specs=(
            P(DP, "mp"),
            P(DP, "mp"),
            P(DP, "mp"),
            P(DP, "mp"),
            P(None, "mp"),
            P(DP, None, "mp"),
        ),
        check_vma=False,
    )
```

```python
import functools

import jax
import jax.numpy as jnp
from jax import lax
from jax.experimental import pallas as pl
from jax.experimental.pallas import tpu as pltpu
from jax.sharding import Mesh
from jax.sharding import PartitionSpec as P

H = 512
BLOCKS = 4
STEP = 10
DP = ("z", "x", "yh", "yl")
NEAR = ("x", "yl")
FAR = ("z", "yh")
SCALE_ONE = 256.0
SCALE_TWO = 32.0
VMEM_LIMIT = 16 * 2**20

beta_one = 0.9
beta_two = 0.95
learn_rate = 0.001
decay_rate = 0.1
epsilon = 1e-08


def dot_over_tokens(rows, cols):
    return lax.dot_general(rows, cols, (((0,), (0,)), ((), ())), preferred_element_type=jnp.float32)


def own_half_kernel(
    flag_ref, mask_ref, normed_ref, cols_ref, stale_ref, part_ref, other_cols_ref, old_ref, fired_ref,
    own, cols, mask, sems
):
    core = lax.axis_index("mp")
    tokens, half_cols = own.shape[0], cols.shape[1]
    copies = [
        pltpu.make_async_copy(cols_ref, cols, sems.at[0]),
        pltpu.make_async_copy(normed_ref, own, sems.at[1]),
        pltpu.make_async_copy(mask_ref, mask, sems.at[2]),
        pltpu.make_async_copy(stale_ref, old_ref, sems.at[3]),
    ]
    for copy in copies:
        copy.start()
    copies[0].wait()
    own_cols = cols[pl.ds(pl.multiple_of(core * tokens, tokens), tokens), :]
    other_cols_ref[...] = cols[pl.ds(pl.multiple_of((1 - core) * tokens, tokens), tokens), :]
    copies[1].wait()
    step = 256
    for at in range(0, own.shape[1], step):
        part_ref[at : at + step, :] = dot_over_tokens(own[:, at : at + step], own_cols)
    copies[2].wait()
    width = H // BLOCKS
    column = lax.broadcasted_iota(jnp.int32, (1, half_cols), 1) + core * half_cols
    fired = jnp.zeros((1, half_cols), jnp.int32)
    for b in range(BLOCKS):
        inside = (column >= b * width) & (column < (b + 1) * width)
        fired = fired + jnp.where(inside, flag_ref[0] * mask[0, b], 0)
    fired_ref[...] = fired.astype(jnp.float32)
    copies[3].wait()


def gradient_kernel(
    sizes, part_ref, other_ref, cols_ref, old_ref, fired_ref, term_ref, kept_ref
):
    nz, nx, nh, nl = sizes
    own_rows = term_ref.shape[1]
    block = nx * nh * nl * own_rows
    fired = fired_ref[...]
    weight = fired * SCALE_ONE
    cols = cols_ref[...]
    for z in range(nz):
        span = slice(z * block, (z + 1) * block)
        grad = part_ref[span, :] + dot_over_tokens(other_ref[:, span], cols)
        old = old_ref[span, :]
        kept_ref[span, :] = jnp.where(fired > 0, grad.astype(jnp.bfloat16), old)
        term = weight * (grad - old.astype(jnp.float32))
        for x in range(nx):
            for yh in range(nh):
                for yl in range(nl):
                    at = ((x * nh + yh) * nl + yl) * own_rows
                    term_ref[((x * nl + yl) * nz + z) * nh + yh] = term[at : at + own_rows, :]


def store_kernel(n_rest, weights_ref, *refs):
    rest, (out_ref, *outs, sems) = refs[:n_rest], refs[n_rest:]
    _, nx, _, nl, _, _ = out_ref.shape
    copies = []
    for x in range(nx):
        for yl in range(nl):
            n = x * nl + yl
            copies.append(
                pltpu.make_async_copy(weights_ref.at[n], out_ref.at[:, x, :, yl], sems.at[n])
            )
    for i in range(n_rest):
        copies.append(pltpu.make_async_copy(rest[i], outs[i], sems.at[nx * nl + i]))
    for copy in copies:
        copy.start()
    for copy in copies:
        copy.wait()


def on_device(
    normed, key_grad, stale, worker_flag, block_mask, aggregate, master, moment_one, moment_two
):
    rows, half_cols = normed.shape[0], key_grad.shape[1]
    d = normed.shape[1]
    other = lax.ppermute(normed, "mp", [(0, 1), (1, 0)])
    sizes = tuple(lax.axis_size(a) for a in DP)
    n_near, n_far = lax.axis_size(NEAR), lax.axis_size(FAR)
    own = d // (n_near * n_far)
    smem = pl.BlockSpec(memory_space=pltpu.SMEM)
    vmem = pl.BlockSpec(memory_space=pltpu.VMEM)
    hbm = pl.BlockSpec(memory_space=pltpu.HBM)
    params = pltpu.CompilerParams(vmem_limit_bytes=VMEM_LIMIT)
    part, other_cols, old, fired = pl.pallas_call(
        own_half_kernel,
        out_shape=(
            jax.ShapeDtypeStruct((d, half_cols), jnp.float32),
            jax.ShapeDtypeStruct((rows, half_cols), jnp.bfloat16),
            jax.ShapeDtypeStruct((d, half_cols), jnp.bfloat16),
            jax.ShapeDtypeStruct((1, half_cols), jnp.float32),
        ),
        in_specs=[smem] + [hbm] * 4,
        out_specs=(vmem,) * 4,
        scratch_shapes=[
            pltpu.VMEM(normed.shape, normed.dtype),
            pltpu.VMEM(key_grad.shape, key_grad.dtype),
            pltpu.SMEM(block_mask.shape, block_mask.dtype),
            pltpu.SemaphoreType.DMA((4,)),
        ],
        compiler_params=params,
    )(
        worker_flag,
        *(
            pltpu.with_memory_space_constraint(a, pltpu.HBM)
            for a in (block_mask, normed, key_grad, stale[0])
        )
    )
    term, kept = pl.pallas_call(
        functools.partial(gradient_kernel, sizes),
        out_shape=(
            jax.ShapeDtypeStruct((d // own, own, half_cols), jnp.float32),
            jax.ShapeDtypeStruct((d, half_cols), jnp.bfloat16),
        ),
        in_specs=[vmem] * 5,
        out_specs=(vmem, vmem),
        compiler_params=params,
    )(part, other, other_cols, old, fired)
    pieces = term.astype(jnp.float16).reshape(n_near, n_far * own, half_cols)
    near = lax.all_to_all(pieces, NEAR, 0, 0, tiled=True)
    partial = jnp.sum(near.astype(jnp.float32), axis=0) * (SCALE_TWO / SCALE_ONE)
    partial = partial.astype(jnp.float16).reshape(n_far, own, half_cols)
    far = lax.all_to_all(partial, FAR, 0, 0, tiled=True)
    reduced = jnp.sum(far.astype(jnp.float32), axis=0) * (1.0 / SCALE_TWO)
    new_aggregate = aggregate + reduced
    new_moment_one = beta_one * moment_one + (1.0 - beta_one) * new_aggregate
    new_moment_two = beta_two * moment_two + (1.0 - beta_two) * new_aggregate * new_aggregate
    first_hat = new_moment_one / (1.0 - beta_one**STEP)
    second_hat = new_moment_two / (1.0 - beta_two**STEP)
    update = first_hat / (jnp.sqrt(second_hat) + epsilon)
    new_master = master - learn_rate * (update + decay_rate * master)
    fresh = new_master.astype(jnp.bfloat16)
    copies = jnp.broadcast_to(fresh, (n_far, own, half_cols))
    block = lax.all_to_all(copies, FAR, 0, 0, tiled=True).reshape(n_far * own, half_cols)
    copies = jnp.broadcast_to(block, (n_near, *block.shape))
    weights = lax.all_to_all(copies, NEAR, 0, 0, tiled=True)
    weights = weights.reshape(n_near, sizes[0], sizes[2], own, half_cols)
    rest = (new_aggregate, new_master, new_moment_one, new_moment_two, kept)
    weights, *rest = pl.pallas_call(
        functools.partial(store_kernel, len(rest)),
        out_shape=(
            jax.ShapeDtypeStruct((*sizes, own, half_cols), jnp.bfloat16),
            *(jax.ShapeDtypeStruct(a.shape, a.dtype) for a in rest),
        ),
        in_specs=[vmem] * (1 + len(rest)),
        out_specs=(hbm,) * (1 + len(rest)),
        scratch_shapes=[pltpu.SemaphoreType.DMA((n_near + len(rest),))],
        compiler_params=params,
    )(weights, *rest)
    return (*rest[:4], weights.reshape(d, half_cols), rest[4][None])


def solution(mesh):
    torus = Mesh(mesh.devices.reshape(8, 4, 4, 2, mesh.shape["mp"]), (*DP, "mp"))
    return jax.shard_map(
        on_device,
        mesh=torus,
        in_specs=(
            P((*DP, "mp"), None),
            P(DP, "mp"),
            P(DP, None, "mp"),
            P(DP),
            P(DP, None),
            P(DP, "mp"),
            P(DP, "mp"),
            P(DP, "mp"),
            P(DP, "mp"),
        ),
        out_specs=(
            P(DP, "mp"),
            P(DP, "mp"),
            P(DP, "mp"),
            P(DP, "mp"),
            P(None, "mp"),
            P(DP, None, "mp"),
        ),
        check_vma=False,
    )
```

```python
import functools

import jax
import jax.numpy as jnp
from jax import lax
from jax.experimental import pallas as pl
from jax.experimental.pallas import tpu as pltpu
from jax.sharding import Mesh
from jax.sharding import PartitionSpec as P

H = 512
BLOCKS = 4
STEP = 10
DP = ("z", "x", "yh", "yl")
NEAR = ("x", "yl")
FAR = ("z", "yh")
SCALE_ONE = 256.0
SCALE_TWO = 32.0
VMEM_LIMIT = 16 * 2**20
LATER_NS = 1000

beta_one = 0.9
beta_two = 0.95
learn_rate = 0.001
decay_rate = 0.1
epsilon = 1e-08


def dot_over_tokens(rows, cols):
    return lax.dot_general(rows, cols, (((0,), (0,)), ((), ())), preferred_element_type=jnp.float32)


def own_half_kernel(
    flag_ref, mask_ref, normed_ref, cols_ref, stale_ref, part_ref, other_cols_ref, old_ref, fired_ref,
    own, cols, mask, sems
):
    core = lax.axis_index("mp")
    tokens, half_cols = own.shape[0], cols.shape[1]
    copies = [
        pltpu.make_async_copy(cols_ref, cols, sems.at[0]),
        pltpu.make_async_copy(normed_ref, own, sems.at[1]),
        pltpu.make_async_copy(mask_ref, mask, sems.at[2]),
        pltpu.make_async_copy(stale_ref, old_ref, sems.at[3]),
    ]
    for copy in copies:
        copy.start()
    copies[0].wait()
    own_cols = cols[pl.ds(pl.multiple_of(core * tokens, tokens), tokens), :]
    other_cols_ref[...] = cols[pl.ds(pl.multiple_of((1 - core) * tokens, tokens), tokens), :]
    copies[1].wait()
    step = 256
    for at in range(0, own.shape[1], step):
        part_ref[at : at + step, :] = dot_over_tokens(own[:, at : at + step], own_cols)
    copies[2].wait()
    width = H // BLOCKS
    column = lax.broadcasted_iota(jnp.int32, (1, half_cols), 1) + core * half_cols
    fired = jnp.zeros((1, half_cols), jnp.int32)
    for b in range(BLOCKS):
        inside = (column >= b * width) & (column < (b + 1) * width)
        fired = fired + jnp.where(inside, flag_ref[0] * mask[0, b], 0)
    fired_ref[...] = fired.astype(jnp.float32)
    copies[3].wait()


def gradient_kernel(
    sizes, part_ref, other_ref, cols_ref, old_ref, fired_ref, term_ref, kept_ref, stored_ref, sem
):
    nz, nx, nh, nl = sizes
    own_rows = term_ref.shape[1]
    block = nx * nh * nl * own_rows
    fired = fired_ref[...]
    weight = fired * SCALE_ONE
    cols = cols_ref[...]
    for z in range(nz):
        span = slice(z * block, (z + 1) * block)
        grad = part_ref[span, :] + dot_over_tokens(other_ref[:, span], cols)
        old = old_ref[span, :]
        kept_ref[span, :] = jnp.where(fired > 0, grad.astype(jnp.bfloat16), old)
        term = weight * (grad - old.astype(jnp.float32))
        for x in range(nx):
            for yh in range(nh):
                for yl in range(nl):
                    at = ((x * nh + yh) * nl + yl) * own_rows
                    term_ref[((x * nl + yl) * nz + z) * nh + yh] = term[at : at + own_rows, :]

    @pl.when(lax.axis_index("mp") == 0)
    def _():
        copy = pltpu.make_async_copy(kept_ref, stored_ref, sem)
        copy.start()
        copy.wait()
        if LATER_NS:
            pl.delay(LATER_NS)


def store_kernel(n_rest, weights_ref, kept_ref, stored_ref, *refs):
    del stored_ref
    rest, (out_ref, stale_ref, *outs, sems) = refs[:n_rest], refs[n_rest:]
    _, nx, _, nl, _, _ = out_ref.shape
    copies = []
    for x in range(nx):
        for yl in range(nl):
            n = x * nl + yl
            copies.append(
                pltpu.make_async_copy(weights_ref.at[n], out_ref.at[:, x, :, yl], sems.at[n])
            )
    for i in range(n_rest):
        copies.append(pltpu.make_async_copy(rest[i], outs[i], sems.at[nx * nl + i]))
    for copy in copies:
        copy.start()

    @pl.when(lax.axis_index("mp") != 0)
    def _():
        copy = pltpu.make_async_copy(kept_ref, stale_ref, sems.at[nx * nl + n_rest])
        copy.start()
        copy.wait()

    for copy in copies:
        copy.wait()


def on_device(
    normed, key_grad, stale, worker_flag, block_mask, aggregate, master, moment_one, moment_two
):
    rows, half_cols = normed.shape[0], key_grad.shape[1]
    d = normed.shape[1]
    other = lax.ppermute(normed, "mp", [(0, 1), (1, 0)])
    sizes = tuple(lax.axis_size(a) for a in DP)
    n_near, n_far = lax.axis_size(NEAR), lax.axis_size(FAR)
    own = d // (n_near * n_far)
    smem = pl.BlockSpec(memory_space=pltpu.SMEM)
    vmem = pl.BlockSpec(memory_space=pltpu.VMEM)
    hbm = pl.BlockSpec(memory_space=pltpu.HBM)
    params = pltpu.CompilerParams(vmem_limit_bytes=VMEM_LIMIT)
    part, other_cols, old, fired = pl.pallas_call(
        own_half_kernel,
        out_shape=(
            jax.ShapeDtypeStruct((d, half_cols), jnp.float32),
            jax.ShapeDtypeStruct((rows, half_cols), jnp.bfloat16),
            jax.ShapeDtypeStruct((d, half_cols), jnp.bfloat16),
            jax.ShapeDtypeStruct((1, half_cols), jnp.float32),
        ),
        in_specs=[smem] + [hbm] * 4,
        out_specs=(vmem,) * 4,
        scratch_shapes=[
            pltpu.VMEM(normed.shape, normed.dtype),
            pltpu.VMEM(key_grad.shape, key_grad.dtype),
            pltpu.SMEM(block_mask.shape, block_mask.dtype),
            pltpu.SemaphoreType.DMA((4,)),
        ],
        compiler_params=params,
    )(
        worker_flag,
        *(
            pltpu.with_memory_space_constraint(a, pltpu.HBM)
            for a in (block_mask, normed, key_grad, stale[0])
        )
    )
    term, kept, stored = pl.pallas_call(
        functools.partial(gradient_kernel, sizes),
        out_shape=(
            jax.ShapeDtypeStruct((d // own, own, half_cols), jnp.float32),
            jax.ShapeDtypeStruct((d, half_cols), jnp.bfloat16),
            pltpu.HBM((d, half_cols), jnp.bfloat16),
        ),
        in_specs=[vmem] * 5,
        out_specs=(vmem, vmem, hbm),
        scratch_shapes=[pltpu.SemaphoreType.DMA(())],
        compiler_params=params,
    )(part, other, other_cols, old, fired)
    pieces = term.astype(jnp.float16).reshape(n_near, n_far * own, half_cols)
    near = lax.all_to_all(pieces, NEAR, 0, 0, tiled=True)
    partial = jnp.sum(near.astype(jnp.float32), axis=0) * (SCALE_TWO / SCALE_ONE)
    partial = partial.astype(jnp.float16).reshape(n_far, own, half_cols)
    far = lax.all_to_all(partial, FAR, 0, 0, tiled=True)
    reduced = jnp.sum(far.astype(jnp.float32), axis=0) * (1.0 / SCALE_TWO)
    new_aggregate = aggregate + reduced
    new_moment_one = beta_one * moment_one + (1.0 - beta_one) * new_aggregate
    new_moment_two = beta_two * moment_two + (1.0 - beta_two) * new_aggregate * new_aggregate
    first_hat = new_moment_one / (1.0 - beta_one**STEP)
    second_hat = new_moment_two / (1.0 - beta_two**STEP)
    update = first_hat / (jnp.sqrt(second_hat) + epsilon)
    new_master = master - learn_rate * (update + decay_rate * master)
    fresh = new_master.astype(jnp.bfloat16)
    copies = jnp.broadcast_to(fresh, (n_far, own, half_cols))
    block = lax.all_to_all(copies, FAR, 0, 0, tiled=True).reshape(n_far * own, half_cols)
    copies = jnp.broadcast_to(block, (n_near, *block.shape))
    weights = lax.all_to_all(copies, NEAR, 0, 0, tiled=True)
    weights = weights.reshape(n_near, sizes[0], sizes[2], own, half_cols)
    rest = (new_aggregate, new_master, new_moment_one, new_moment_two)
    weights, new_stale, *rest = pl.pallas_call(
        functools.partial(store_kernel, len(rest)),
        out_shape=(
            jax.ShapeDtypeStruct((*sizes, own, half_cols), jnp.bfloat16),
            pltpu.HBM(kept.shape, kept.dtype),
            *(jax.ShapeDtypeStruct(a.shape, a.dtype) for a in rest),
        ),
        in_specs=[vmem, vmem, hbm] + [vmem] * len(rest),
        out_specs=(hbm,) * (2 + len(rest)),
        input_output_aliases={2: 1},
        scratch_shapes=[pltpu.SemaphoreType.DMA((n_near + len(rest) + 1,))],
        compiler_params=params,
    )(weights, kept, stored, *rest)
    return (*rest, weights.reshape(d, half_cols), new_stale[None])


def solution(mesh):
    torus = Mesh(mesh.devices.reshape(8, 4, 4, 2, mesh.shape["mp"]), (*DP, "mp"))
    return jax.shard_map(
        on_device,
        mesh=torus,
        in_specs=(
            P((*DP, "mp"), None),
            P(DP, "mp"),
            P(DP, None, "mp"),
            P(DP),
            P(DP, None),
            P(DP, "mp"),
            P(DP, "mp"),
            P(DP, "mp"),
            P(DP, "mp"),
        ),
        out_specs=(
            P(DP, "mp"),
            P(DP, "mp"),
            P(DP, "mp"),
            P(DP, "mp"),
            P(None, "mp"),
            P(DP, None, "mp"),
        ),
        check_vma=False,
    )
```

```python
import functools

import jax
import jax.numpy as jnp
from jax import lax
from jax.experimental import pallas as pl
from jax.experimental.pallas import tpu as pltpu
from jax.sharding import Mesh
from jax.sharding import PartitionSpec as P

H = 512
BLOCKS = 4
STEP = 10
DP = ("z", "x", "yh", "yl")
NEAR = ("x", "yl")
FAR = ("z", "yh")
SCALE_ONE = 256.0
SCALE_TWO = 32.0
VMEM_LIMIT = 16 * 2**20
LATER_NS = 1000

beta_one = 0.9
beta_two = 0.95
learn_rate = 0.001
decay_rate = 0.1
epsilon = 1e-08


def dot_over_tokens(rows, cols):
    return lax.dot_general(rows, cols, (((0,), (0,)), ((), ())), preferred_element_type=jnp.float32)


def own_half_kernel(
    flag_ref, mask_ref, normed_ref, cols_ref, stale_ref, part_ref, other_cols_ref, old_ref, fired_ref,
    own, cols, mask, sems
):
    core = lax.axis_index("mp")
    tokens, half_cols = own.shape[0], cols.shape[1]
    copies = [
        pltpu.make_async_copy(cols_ref, cols, sems.at[0]),
        pltpu.make_async_copy(normed_ref, own, sems.at[1]),
        pltpu.make_async_copy(mask_ref, mask, sems.at[2]),
        pltpu.make_async_copy(stale_ref, old_ref, sems.at[3]),
    ]
    for copy in copies:
        copy.start()
    copies[0].wait()
    own_cols = cols[pl.ds(pl.multiple_of(core * tokens, tokens), tokens), :]
    other_cols_ref[...] = cols[pl.ds(pl.multiple_of((1 - core) * tokens, tokens), tokens), :]
    copies[1].wait()
    step = 1024
    for at in range(0, own.shape[1], step):
        part_ref[at : at + step, :] = dot_over_tokens(own[:, at : at + step], own_cols)
    copies[2].wait()
    width = H // BLOCKS
    column = lax.broadcasted_iota(jnp.int32, (1, half_cols), 1) + core * half_cols
    fired = jnp.zeros((1, half_cols), jnp.int32)
    for b in range(BLOCKS):
        inside = (column >= b * width) & (column < (b + 1) * width)
        fired = fired + jnp.where(inside, flag_ref[0] * mask[0, b], 0)
    fired_ref[...] = fired.astype(jnp.float32)
    copies[3].wait()


def gradient_kernel(
    sizes, part_ref, other_ref, cols_ref, old_ref, fired_ref, term_ref, kept_ref, stored_ref, sem
):
    nz, nx, nh, nl = sizes
    own_rows = term_ref.shape[1]
    block = nx * nh * nl * own_rows
    fired = fired_ref[...]
    weight = fired * SCALE_ONE
    cols = cols_ref[...]
    for z in range(nz):
        span = slice(z * block, (z + 1) * block)
        grad = part_ref[span, :] + dot_over_tokens(other_ref[:, span], cols)
        old = old_ref[span, :]
        kept_ref[span, :] = jnp.where(fired > 0, grad.astype(jnp.bfloat16), old)
        term = weight * (grad - old.astype(jnp.float32))
        for x in range(nx):
            for yh in range(nh):
                for yl in range(nl):
                    at = ((x * nh + yh) * nl + yl) * own_rows
                    term_ref[((x * nl + yl) * nz + z) * nh + yh] = term[at : at + own_rows, :]

    @pl.when(lax.axis_index("mp") == 0)
    def _():
        copy = pltpu.make_async_copy(kept_ref, stored_ref, sem)
        copy.start()
        copy.wait()
        if LATER_NS:
            pl.delay(LATER_NS)


def store_kernel(n_rest, weights_ref, kept_ref, stored_ref, *refs):
    del stored_ref
    rest, (out_ref, stale_ref, *outs, sems) = refs[:n_rest], refs[n_rest:]
    _, nx, _, nl, _, _ = out_ref.shape
    copies = []
    for x in range(nx):
        for yl in range(nl):
            n = x * nl + yl
            copies.append(
                pltpu.make_async_copy(weights_ref.at[n], out_ref.at[:, x, :, yl], sems.at[n])
            )
    for i in range(n_rest):
        copies.append(pltpu.make_async_copy(rest[i], outs[i], sems.at[nx * nl + i]))
    for copy in copies:
        copy.start()

    @pl.when(lax.axis_index("mp") != 0)
    def _():
        copy = pltpu.make_async_copy(kept_ref, stale_ref, sems.at[nx * nl + n_rest])
        copy.start()
        copy.wait()

    for copy in copies:
        copy.wait()


def on_device(
    normed, key_grad, stale, worker_flag, block_mask, aggregate, master, moment_one, moment_two
):
    rows, half_cols = normed.shape[0], key_grad.shape[1]
    d = normed.shape[1]
    other = lax.ppermute(normed, "mp", [(0, 1), (1, 0)])
    sizes = tuple(lax.axis_size(a) for a in DP)
    n_near, n_far = lax.axis_size(NEAR), lax.axis_size(FAR)
    own = d // (n_near * n_far)
    smem = pl.BlockSpec(memory_space=pltpu.SMEM)
    vmem = pl.BlockSpec(memory_space=pltpu.VMEM)
    hbm = pl.BlockSpec(memory_space=pltpu.HBM)
    params = pltpu.CompilerParams(vmem_limit_bytes=VMEM_LIMIT)
    part, other_cols, old, fired = pl.pallas_call(
        own_half_kernel,
        out_shape=(
            jax.ShapeDtypeStruct((d, half_cols), jnp.float32),
            jax.ShapeDtypeStruct((rows, half_cols), jnp.bfloat16),
            jax.ShapeDtypeStruct((d, half_cols), jnp.bfloat16),
            jax.ShapeDtypeStruct((1, half_cols), jnp.float32),
        ),
        in_specs=[smem] + [hbm] * 4,
        out_specs=(vmem,) * 4,
        scratch_shapes=[
            pltpu.VMEM(normed.shape, normed.dtype),
            pltpu.VMEM(key_grad.shape, key_grad.dtype),
            pltpu.SMEM(block_mask.shape, block_mask.dtype),
            pltpu.SemaphoreType.DMA((4,)),
        ],
        compiler_params=params,
    )(
        worker_flag,
        *(
            pltpu.with_memory_space_constraint(a, pltpu.HBM)
            for a in (block_mask, normed, key_grad, stale[0])
        )
    )
    term, kept, stored = pl.pallas_call(
        functools.partial(gradient_kernel, sizes),
        out_shape=(
            jax.ShapeDtypeStruct((d // own, own, half_cols), jnp.float32),
            jax.ShapeDtypeStruct((d, half_cols), jnp.bfloat16),
            pltpu.HBM((d, half_cols), jnp.bfloat16),
        ),
        in_specs=[vmem] * 5,
        out_specs=(vmem, vmem, hbm),
        scratch_shapes=[pltpu.SemaphoreType.DMA(())],
        compiler_params=params,
    )(part, other, other_cols, old, fired)
    pieces = term.astype(jnp.float16).reshape(n_near, n_far * own, half_cols)
    near = lax.all_to_all(pieces, NEAR, 0, 0, tiled=True)
    partial = jnp.sum(near.astype(jnp.float32), axis=0) * (SCALE_TWO / SCALE_ONE)
    partial = partial.astype(jnp.float16).reshape(n_far, own, half_cols)
    far = lax.all_to_all(partial, FAR, 0, 0, tiled=True)
    reduced = jnp.sum(far.astype(jnp.float32), axis=0) * (1.0 / SCALE_TWO)
    new_aggregate = aggregate + reduced
    new_moment_one = beta_one * moment_one + (1.0 - beta_one) * new_aggregate
    new_moment_two = beta_two * moment_two + (1.0 - beta_two) * new_aggregate * new_aggregate
    first_hat = new_moment_one / (1.0 - beta_one**STEP)
    second_hat = new_moment_two / (1.0 - beta_two**STEP)
    update = first_hat / (jnp.sqrt(second_hat) + epsilon)
    new_master = master - learn_rate * (update + decay_rate * master)
    fresh = new_master.astype(jnp.bfloat16)
    copies = jnp.broadcast_to(fresh, (n_far, own, half_cols))
    block = lax.all_to_all(copies, FAR, 0, 0, tiled=True).reshape(n_far * own, half_cols)
    copies = jnp.broadcast_to(block, (n_near, *block.shape))
    weights = lax.all_to_all(copies, NEAR, 0, 0, tiled=True)
    weights = weights.reshape(n_near, sizes[0], sizes[2], own, half_cols)
    rest = (new_aggregate, new_master, new_moment_one, new_moment_two)
    weights, new_stale, *rest = pl.pallas_call(
        functools.partial(store_kernel, len(rest)),
        out_shape=(
            jax.ShapeDtypeStruct((*sizes, own, half_cols), jnp.bfloat16),
            pltpu.HBM(kept.shape, kept.dtype),
            *(jax.ShapeDtypeStruct(a.shape, a.dtype) for a in rest),
        ),
        in_specs=[vmem, vmem, hbm] + [vmem] * len(rest),
        out_specs=(hbm,) * (2 + len(rest)),
        input_output_aliases={2: 1},
        scratch_shapes=[pltpu.SemaphoreType.DMA((n_near + len(rest) + 1,))],
        compiler_params=params,
    )(weights, kept, stored, *rest)
    return (*rest, weights.reshape(d, half_cols), new_stale[None])


def solution(mesh):
    torus = Mesh(mesh.devices.reshape(8, 4, 4, 2, mesh.shape["mp"]), (*DP, "mp"))
    return jax.shard_map(
        on_device,
        mesh=torus,
        in_specs=(
            P((*DP, "mp"), None),
            P(DP, "mp"),
            P(DP, None, "mp"),
            P(DP),
            P(DP, None),
            P(DP, "mp"),
            P(DP, "mp"),
            P(DP, "mp"),
            P(DP, "mp"),
        ),
        out_specs=(
            P(DP, "mp"),
            P(DP, "mp"),
            P(DP, "mp"),
            P(DP, "mp"),
            P(None, "mp"),
            P(DP, None, "mp"),
        ),
        check_vma=False,
    )
```
